32 devices in a mesh: pass: 8 (over z, x), cell: 4 (over y, core).
Axes of the slice: x: 2, y: 2, z: 4, core: 2. Of those that a mesh axis runs over, the one named last changes fastest.
Arguments:
- flow_state: float32 [2048, 4096], P('pass', 'cell'), may hold values from -6 to 6
- face_weights: float32 [4, 2048, 4096], P(None, 'pass', 'cell'), may hold values from 0.02 to 0.24
- forcing: float32 [2048, 4096], P('pass', 'cell'), may hold values from -1.2 to 1.2
- lagged_planes: float32 [8, 8, 4096], P('pass', None, 'cell'), may hold values from -6 to 6
- phase_lag: int32 [4, 2], replicated, may hold values from 0 to 8
- face_map: int32 [8, 4096], P('pass', 'cell'), may hold values from 0 to 4095, as said below
- surface_record: bfloat16 [8, 120, 4096], P('pass', None, 'cell'), may hold values from -6 to 6
- face_radius: float32 [2, 4096], P(None, 'cell'), may hold values from 0.3 to 1
- face_angle: float32 [2, 4096], P(None, 'cell'), may hold values from -0.3 to 0.3
- face_axial: float32 [2, 4096], P(None, 'cell'), may hold values from -0.3 to 0.3
- face_stagger: float32 [2, 4096], P(None, 'cell'), may hold values from -1.2 to 1.2
- face_area: float32 [2, 4096], P(None, 'cell'), may hold values from 0.5 to 1.5
- listeners: float32 [3, 1024], replicated, as said below
- observer_group: int32 [1024], replicated, may hold values from 0 to 15
Outputs:
- final_field: float32 [2048, 4096], P('pass', 'cell')
- acoustic: float32 [1024, 128], P('cell')
- array_signal: float32 [16, 128], replicated
The draws below stay inside these ranges and needn't reach their ends.
Inputs may be any that keep to these rules, and one draw needn't show every extreme that they name: face_map[j, a] lies in the aligned block of 1024 axial indices that holds a, and for each j the entries of a block are a permutation of that block. `listeners`: every observer is between 1.3 and 4 from the anchor.
All inputs are finite; a program needn't handle non-finite values.
Results may differ from the reference program's by a relative error of at most 0.0035.
Values sent between devices are 32-bit elements; how exact they have to be, the bound alone decides.
A program may use at most 64 MiB of HBM per device.

```python
import math
import jax
import jax.numpy as jnp
from jax import lax

CA = 1024
PITCH = 512
OBS = 1024
TIMES = 128
STEPS = 8
LAGS = 8
GROUPS = 16
PASSAGES = 4
A = 4096


def draw_face_map(key, part):
    blocks = A // CA
    scores = jax.random.randint(key, (2 * PASSAGES, blocks, CA), 0, 65536)
    scores = scores * CA + jnp.arange(CA, dtype=jnp.int32)
    order = jnp.argsort(scores, axis=-1, stable=True).astype(jnp.int32)
    offsets = (jnp.arange(blocks, dtype=jnp.int32) * CA)[None, :, None]
    return (order + offsets).reshape(2 * PASSAGES, A).astype(jnp.int32)


def draw_listeners(key, part):
    first, second, third = jax.random.split(key, 3)
    polar = jax.random.uniform(first, (OBS,), jnp.float32, -1.0, 1.0)
    radius = jax.random.uniform(third, (OBS,), jnp.float32, 1.3, 4.0)
    azimuth = jax.random.uniform(second, (OBS,), jnp.float32, -math.pi, math.pi)
    lateral = jnp.sqrt(jnp.maximum(1.0 - polar * polar, 0.0))
    return jnp.stack([radius * lateral * jnp.cos(azimuth), radius * lateral * jnp.sin(azimuth), radius * polar]).astype(jnp.float32)


def set_ends(array, rng, smallest, largest):
    dims = array.shape
    index_at = [jax.random.randint(jax.random.fold_in(rng, axis), (), 0, dims[axis]) for axis in range(len(dims))]
    array = array.at[tuple(index_at)].set(smallest)
    longest = dims.index(max(dims))
    index_at[longest] = (index_at[longest] + 1) % dims[longest]
    return array.at[tuple(index_at)].set(largest)


def shard_levels(stream_key, shape, cuts, smallest, high):
    level, own = 1.0, jax.random.fold_in(stream_key, 6)
    for position, parts in cuts:
        heights = jnp.exp(jax.random.uniform(jax.random.fold_in(own, position), (parts,), jnp.float32, smallest / len(cuts), high / len(cuts)))
        level = level * jnp.repeat(heights, shape[position] // parts).reshape([-1 if axis == position else 1 for axis in range(len(shape))])
    return level


def bell_draw(rng, extent, spread, bound, cuts=(), kind=jnp.bfloat16):
    array = spread * jax.random.normal(rng, extent, jnp.float32)
    if cuts:
        array = array * shard_levels(rng, extent, cuts, -0.22, 0.18)
    return jnp.clip(array, -bound, bound).astype(kind)


def setup_inputs(seed: int = 0) -> dict:
    splits = jax.random.split(jax.random.key(seed), 15)
    return {
        "flow_state": bell_draw(splits[0], (PASSAGES * PITCH, A), 1.0, 6.0, ((0, 8), (1, 4)), jnp.float32),
        "face_weights": jnp.clip(0.02 + 0.22 * jax.random.uniform(splits[1], (4, PASSAGES * PITCH, A), jnp.float32) ** shard_levels(splits[1], (4, PASSAGES * PITCH, A), ((1, 8), (2, 4)), -0.2, 0.2), 0.02, 0.24),
        "forcing": bell_draw(splits[2], (PASSAGES * PITCH, A), 0.2, 1.2, ((0, 8), (1, 4)), jnp.float32),
        "lagged_planes": bell_draw(splits[3], (2 * PASSAGES, LAGS, A), 1.0, 6.0, ((0, 8), (2, 4)), jnp.float32),
        "phase_lag": set_ends(jax.random.randint(splits[4], (PASSAGES, 2), 0, LAGS + 1), jax.random.fold_in(splits[4], 1), 0, LAGS).astype(jnp.int32),
        "face_map": draw_face_map(jax.random.fold_in(splits[14], 71), 0),
        "surface_record": bell_draw(splits[6], (2 * PASSAGES, TIMES - STEPS, A), 1.0, 6.0, ((0, 8), (2, 4))),
        "face_radius": jnp.clip(0.3 + 0.7 * jax.random.uniform(splits[7], (2, A), jnp.float32) ** shard_levels(splits[7], (2, A), ((1, 4),), -0.2, 0.2), 0.3, 1.0),
        "face_angle": jnp.clip(jax.random.uniform(splits[8], (2, A), jnp.float32, -0.3, 0.3) * shard_levels(splits[8], (2, A), ((1, 4),), -0.4, 0.0), -0.3, 0.3),
        "face_axial": jnp.clip(jax.random.uniform(splits[9], (2, A), jnp.float32, -0.3, 0.3) * shard_levels(splits[9], (2, A), ((1, 4),), -0.4, 0.0), -0.3, 0.3),
        "face_stagger": jnp.clip(jax.random.uniform(splits[10], (2, A), jnp.float32, -1.2, 1.2) * shard_levels(splits[10], (2, A), ((1, 4),), -0.4, 0.0), -1.2, 1.2),
        "face_area": jnp.clip(0.5 + 1.0 * jax.random.uniform(splits[11], (2, A), jnp.float32) ** shard_levels(splits[11], (2, A), ((1, 4),), -0.2, 0.2), 0.5, 1.5),
        "listeners": draw_listeners(jax.random.fold_in(splits[14], 71), 0),
        "observer_group": set_ends(jax.random.randint(splits[13], (OBS,), 0, GROUPS), jax.random.fold_in(splits[13], 1), 0, GROUPS - 1).astype(jnp.int32),
    }


sound_speed = 2.0

def relax(field, coeff, forcing, ghost_low, ghost_high):
    below = jnp.concatenate([ghost_low[:, None, :], field[:, :-1, :]], axis=1)
    above = jnp.concatenate([field[:, 1:, :], ghost_high[:, None, :]], axis=1)
    border = jnp.zeros_like(field[:, :, :1])
    left = jnp.concatenate([border, field[:, :, :-1]], axis=2)
    right = jnp.concatenate([field[:, :, 1:], border], axis=2)
    keep = 1.0 - coeff[0] - coeff[1] - coeff[2] - coeff[3]
    return keep * field + coeff[0] * below + coeff[1] * above + coeff[2] * left + coeff[3] * right + forcing

def pick_level(levels, lag, mapping):
    count = levels.shape[1]
    width = levels.shape[2]
    index = jnp.broadcast_to(lag[None, :, None], (1, count, width)).astype(jnp.int32)
    chosen = jnp.take_along_axis(levels, index, axis=0)[0]
    return jnp.take_along_axis(chosen, mapping.astype(jnp.int32), axis=1)

def time_rate(signal, axis):
    values = signal.astype(jnp.float32)
    length = values.shape[axis]
    inner = (lax.slice_in_dim(values, 2, length, axis=axis) - lax.slice_in_dim(values, 0, length - 2, axis=axis)) * 0.5
    head = lax.slice_in_dim(values, 1, 2, axis=axis) - lax.slice_in_dim(values, 0, 1, axis=axis)
    tail = lax.slice_in_dim(values, length - 1, length, axis=axis) - lax.slice_in_dim(values, length - 2, length - 1, axis=axis)
    return jnp.concatenate([head, inner, tail], axis=axis).astype(jnp.bfloat16)

def kernel_pair(points, theta, radius, angle, axial, stagger, area, scale):
    phase = theta + angle
    cos_phase = jnp.cos(phase)
    sin_phase = jnp.sin(phase)
    normal_x = -jnp.cos(stagger) * sin_phase
    normal_y = jnp.cos(stagger) * cos_phase
    normal_z = jnp.sin(stagger)
    delta_x = points[0][:, None] - (radius * cos_phase)[None, :]
    delta_y = points[1][:, None] - (radius * sin_phase)[None, :]
    delta_z = points[2][:, None] - axial[None, :]
    dist_sq = delta_x * delta_x + delta_y * delta_y + delta_z * delta_z
    dist = jnp.sqrt(dist_sq)
    cosine = (normal_x[None, :] * delta_x + normal_y[None, :] * delta_y + normal_z[None, :] * delta_z) / dist
    weight = (area * scale / (4.0 * math.pi))[None, :] * cosine
    press = (weight / dist_sq).astype(jnp.bfloat16)
    change = (weight / (sound_speed * dist)).astype(jnp.bfloat16)
    return jnp.concatenate([press, change], axis=1)

def reference(flow_state, face_weights, forcing, lagged_planes, phase_lag, face_map, surface_record, face_radius, face_angle, face_axial, face_stagger, face_area, listeners, observer_group):
    field = flow_state.reshape(PASSAGES, PITCH, A)
    coeff = face_weights.reshape(4, PASSAGES, PITCH, A)
    push = forcing.reshape(PASSAGES, PITCH, A)
    planes = lagged_planes.reshape(PASSAGES, 2, LAGS, A)
    maps = face_map.reshape(PASSAGES, 2, A)
    lower_levels = jnp.concatenate([field[None, :, 0, :], jnp.moveaxis(planes[:, 0], 1, 0)], axis=0)
    upper_levels = jnp.concatenate([field[None, :, -1, :], jnp.moveaxis(planes[:, 1], 1, 0)], axis=0)
    surfaces = []
    for level in range(STEPS):
        ghost_low = pick_level(jnp.roll(upper_levels, 1, axis=1), phase_lag[:, 0], maps[:, 0, :])
        ghost_high = pick_level(jnp.roll(lower_levels, -1, axis=1), phase_lag[:, 1], maps[:, 1, :])
        field = relax(field, coeff, push, ghost_low, ghost_high)
        lower_levels = jnp.concatenate([field[None, :, 0, :], lower_levels[:-1]], axis=0)
        upper_levels = jnp.concatenate([field[None, :, -1, :], upper_levels[:-1]], axis=0)
        sides = jnp.stack([field[:, PITCH // 4, :], field[:, PITCH // 4 + PITCH // 2, :]], axis=1)
        surfaces.append(sides.reshape(2 * PASSAGES, A).astype(jnp.bfloat16))
    surface = jnp.concatenate([surface_record, jnp.stack(surfaces, axis=1)], axis=1)
    rate = time_rate(surface, 1)
    rows = jnp.arange(2 * PASSAGES, dtype=jnp.int32)
    thetas = (rows // 2).astype(jnp.float32) * (2.0 * math.pi / PASSAGES)
    side_ids = (rows % 2).astype(jnp.int32)
    scale = 64.0 / math.sqrt(2 * A * PASSAGES)

    def passage_term(operands):
        signal, change, theta, side = operands
        kernel = kernel_pair(listeners, theta, face_radius[side], face_angle[side], face_axial[side], face_stagger[side], face_area[side], scale)
        data = jnp.concatenate([signal, change], axis=1)
        return jnp.dot(kernel, data.T, preferred_element_type=jnp.float32)
    terms = lax.map(passage_term, (surface, rate, thetas, side_ids))
    acoustic = lax.optimization_barrier(jnp.sum(terms, axis=0))
    member = (observer_group[None, :] == jnp.arange(GROUPS, dtype=jnp.int32)[:, None]).astype(jnp.float32)
    counts = lax.optimization_barrier(jnp.sum(member, axis=1))
    totals = jnp.dot(member, acoustic, precision=lax.Precision.HIGHEST, preferred_element_type=jnp.float32)
    array_signal = totals / jnp.maximum(counts, 1.0)[:, None]
    return (field.reshape(PASSAGES * PITCH, A), acoustic, array_signal)
```

```python
import functools
import math

import jax
import jax.numpy as jnp
from jax import lax
from jax.experimental import pallas as pl
from jax.experimental.pallas import tpu as pltpu
from jax.sharding import PartitionSpec as P

STEPS = 8
GROUPS = 16
SOUND = 2.0
MESH = pl.DeviceIdType.MESH
F32 = jnp.float32
BF16 = jnp.bfloat16


def fold(row):
    width = row.shape[1]
    return jnp.concatenate([row[:, i : i + 128] for i in range(0, width, 128)], axis=0)


def unfold(slab):
    return jnp.concatenate([slab[i : i + 1, :] for i in range(slab.shape[0])], axis=1)


def iota(shape, dim):
    return lax.broadcasted_iota(jnp.int32, shape, dim)


def body(
    passes,
    cells,
    lag_ref,
    u_in,
    w_ref,
    f_ref,
    planes_ref,
    map_ref,
    record_ref,
    radius_ref,
    angle_ref,
    axial_ref,
    stagger_ref,
    area_ref,
    points_ref,
    group_ref,
    field_out,
    acoustic_out,
    array_out,
    u,
    keep,
    low_hist,
    up_hist,
    row_send,
    row_recv,
    col_send,
    col_recv,
    rim,
    surf,
    rate,
    faces,
    press,
    change,
    part_send,
    part_recv,
    sum_send,
    sum_recv,
    own,
    gathered,
    row_ssem,
    row_rsem,
    col_ssem,
    col_rsem,
    part_ssem,
    part_rsem,
    sum_ssem,
    sum_rsem,
    all_ssem,
    all_rsem,
):
    p = lax.axis_index("pass")
    c = lax.axis_index("cell")
    height, width = u_in.shape
    half = lax.rem(p, 2)
    passage = lax.div(p, 2)
    count = passes // 2
    lags = planes_ref.shape[1]
    observers = points_ref.shape[1]
    records = record_ref.shape[1]

    def pass_peer(d):
        return (lax.rem(p + d, passes), c)

    def cell_peer(d):
        return (p, lax.rem(c + d, cells))

    barrier = pltpu.get_barrier_semaphore()
    for d in range(1, cells):
        pl.semaphore_signal(barrier, inc=1, device_id=cell_peer(d), device_id_type=MESH)

    @pl.loop(1, passes)
    def _(d):
        pl.semaphore_signal(barrier, inc=1, device_id=pass_peer(d), device_id_type=MESH)

    after_lag = lag_ref[lax.rem(passage + 1, count), 0]
    before_lag = lag_ref[lax.rem(passage + count - 1, count), 1]
    up_pick = jnp.where(half == 1, after_lag, 0)
    down_pick = jnp.where(half == 0, before_lag, 0)

    def row_copy(level, way):
        d = 1 if way == 0 else passes - 1
        return pltpu.make_async_remote_copy(
            src_ref=row_send.at[level, way],
            dst_ref=row_recv.at[level, way],
            send_sem=row_ssem.at[level, way],
            recv_sem=row_rsem.at[level, way],
            device_id=pass_peer(d),
            device_id_type=MESH,
        )

    def col_copy(level, way):
        d = 1 if way == 0 else cells - 1
        return pltpu.make_async_remote_copy(
            src_ref=col_send.at[level, way],
            dst_ref=col_recv.at[level, way],
            send_sem=col_ssem.at[level, way],
            recv_sem=col_rsem.at[level, way],
            device_id=cell_peer(d),
            device_id_type=MESH,
        )

    def send_rows(level):
        row_send[level, 0] = fold(up_hist[pl.ds(lags + level - up_pick, 1), :])
        row_send[level, 1] = fold(low_hist[pl.ds(lags + level - down_pick, 1), :])
        row_copy(level, 0).start()
        row_copy(level, 1).start()

    lane = iota((128, 128), 1)
    sub = iota((128, 128), 0)

    def send_cols(level, first, last):
        for k in range(height // 128):
            rows = pl.ds(k * 128, 128)
            both = jnp.where(lane == 127, last(rows), first(rows)).T
            col_send[level, 1, k : k + 1, :] = both[0:1, :]
            col_send[level, 0, k : k + 1, :] = both[127:128, :]
        col_copy(level, 0).start()
        col_copy(level, 1).start()

    for j in range(lags):
        low_hist[lags - 1 - j : lags - j, :] = planes_ref[0, j : j + 1, :]
        up_hist[lags - 1 - j : lags - j, :] = planes_ref[0, j : j + 1, :]
    low_hist[lags : lags + 1, :] = u_in[0:1, :]
    up_hist[lags : lags + 1, :] = u_in[height - 1 : height, :]

    pl.semaphore_wait(barrier, cells - 1 + passes - 1)
    send_rows(0)
    send_cols(0, lambda rows: u_in[rows, 0:128], lambda rows: u_in[rows, width - 128 : width])

    @pl.loop(0, height // 8)
    def _(i):
        rows = pl.ds(pl.multiple_of(i * 8, 8), 8)
        u[0, rows, :] = u_in[rows, :]
        keep[rows, :] = (
            1.0 - w_ref[0, rows, :] - w_ref[1, rows, :] - w_ref[2, rows, :] - w_ref[3, rows, :]
        )

    local_map = fold(map_ref[...]) - c * width
    map_row = lax.div(local_map, 128)
    map_lane = lax.rem(local_map, 128)

    surf[0:records, :] = record_ref[0].astype(F32)
    theta = passage.astype(F32) * (2.0 * math.pi / count)
    scale = 64.0 / math.sqrt(width * cells * passes)
    mine = pl.ds(half, 1)
    phase = theta + fold(angle_ref[mine, :])
    cos_phase = jnp.cos(phase)
    sin_phase = jnp.sin(phase)
    stagger = fold(stagger_ref[mine, :])
    cos_stagger = jnp.cos(stagger)
    sin_stagger = jnp.sin(stagger)
    radius = fold(radius_ref[mine, :])
    weight = fold(area_ref[mine, :]) * (scale / (4.0 * math.pi))
    faces[0] = radius * cos_phase
    faces[1] = radius * sin_phase
    faces[2] = fold(axial_ref[mine, :])
    faces[3] = -cos_stagger * sin_phase * weight
    faces[4] = cos_stagger * cos_phase * weight
    faces[5] = sin_stagger * weight

    lane8 = iota((8, 128), 1)
    sub8 = iota((8, width), 0)

    def block(src, dst, start, before, after):
        rows = pl.ds(start, 8)
        now = u[src, rows, :]
        edge = rim[rows, :]
        below = jnp.where(sub8 == 0, before, pltpu.roll(now, 1, 0))
        above = jnp.where(sub8 == 7, after, pltpu.roll(now, 7, 0))
        left = pltpu.roll(now, 1, 1)
        right = pltpu.roll(now, width - 1, 1)
        left = jnp.concatenate(
            [jnp.where(lane8 == 0, edge, left[:, :128]), left[:, 128:]], axis=1
        )
        right = jnp.concatenate(
            [right[:, : width - 128], jnp.where(lane8 == 127, edge, right[:, width - 128 :])],
            axis=1,
        )
        value = (
            keep[rows, :] * now
            + w_ref[0, rows, :] * below
            + w_ref[1, rows, :] * above
            + w_ref[2, rows, :] * left
            + w_ref[3, rows, :] * right
            + f_ref[rows, :]
        )
        u[dst, rows, :] = value
        return value

    chunk = observers // STEPS

    def kernels(step):
        @pl.loop(0, chunk // 128)
        def _(k):
            base = pl.multiple_of(step * chunk + k * 128, 128)
            xyz = [
                jnp.broadcast_to(points_ref[i : i + 1, pl.ds(base, 128)], (128, 128)).T
                for i in range(3)
            ]
            for j in range(width // 128):
                row = [faces[i, j : j + 1, :] for i in range(6)]
                for s in range(0, 128, 32):
                    dx = xyz[0][s : s + 32] - row[0]
                    dy = xyz[1][s : s + 32] - row[1]
                    dz = xyz[2][s : s + 32] - row[2]
                    inv = lax.rsqrt(dx * dx + dy * dy + dz * dz)
                    dot = row[3] * dx + row[4] * dy + row[5] * dz
                    q = dot * (inv * inv)
                    at = (pl.ds(base + s, 32), pl.ds(j * 128, 128))
                    press[at] = (q * inv).astype(BF16)
                    change[at] = (q * (1.0 / SOUND)).astype(BF16)

    @pl.loop(0, STEPS)
    def _(m):
        src = lax.rem(m, 2)
        dst = 1 - src
        for way in range(2):
            col_copy(m, way).wait_recv()
        col_l = jnp.where(c > 0, col_recv[m, 0], 0.0)
        col_r = jnp.where(c < cells - 1, col_recv[m, 1], 0.0)
        for k in range(height // 128):
            rim[k * 128 : (k + 1) * 128, :] = jnp.where(
                sub < 64, col_l[k : k + 1, :], col_r[k : k + 1, :]
            ).T
        for way in range(2):
            row_copy(m, way).wait_recv()
        raw_low = row_recv[m, 0]
        raw_high = row_recv[m, 1]
        raw = jnp.where(half == 0, raw_low, raw_high)
        mapped = jnp.zeros_like(raw)
        for s in range(width // 128):
            picked = jnp.take_along_axis(
                jnp.broadcast_to(raw[s : s + 1, :], raw.shape),
                map_lane,
                axis=1,
                mode="promise_in_bounds",
            )
            mapped = jnp.where(map_row == s, picked, mapped)
        ghost_low = unfold(jnp.where(half == 0, mapped, raw_low))
        ghost_high = unfold(jnp.where(half == 1, mapped, raw_high))
        first = block(src, dst, 0, ghost_low, pltpu.roll(u[src, 8:16, :], 7, 0))
        last = block(
            src, dst, height - 8, pltpu.roll(u[src, height - 16 : height - 8, :], 1, 0), ghost_high
        )
        low_hist[pl.ds(lags + m + 1, 1), :] = first[0:1, :]
        up_hist[pl.ds(lags + m + 1, 1), :] = last[7:8, :]

        @pl.when(m < STEPS - 1)
        def _():
            send_rows(m + 1)

        @pl.loop(1, height // 8 - 1, unroll=2)
        def _(i):
            start = pl.multiple_of(i * 8, 8)
            before = pltpu.roll(u[src, pl.ds(pl.multiple_of(start - 8, 8), 8), :], 1, 0)
            after = pltpu.roll(u[src, pl.ds(pl.multiple_of(start + 8, 8), 8), :], 7, 0)
            block(src, dst, start, before, after)

        @pl.when(m < STEPS - 1)
        def _():
            send_cols(
                m + 1,
                lambda rows: u[dst, rows, 0:128],
                lambda rows: u[dst, rows, width - 128 : width],
            )

        side = u[dst, height // 2 : height // 2 + 1, :]
        surf[pl.ds(records + m, 1), :] = side.astype(BF16).astype(F32)
        kernels(m)

    times = records + STEPS
    for j in range(width // 128):
        cols = slice(j * 128, (j + 1) * 128)
        v = surf[:, cols]
        tt = iota(v.shape, 0)
        nxt = pltpu.roll(v, times - 1, 0)
        prv = pltpu.roll(v, 1, 0)
        r = jnp.where(
            tt == 0, nxt - v, jnp.where(tt == times - 1, v - prv, (nxt - prv) * 0.5)
        )
        rate[0, :, cols] = v.astype(BF16)
        rate[1, :, cols] = r.astype(BF16)

    per = observers // cells
    total = jnp.zeros((GROUPS, times), F32)
    label = iota((GROUPS, per), 0)
    members = jnp.zeros((GROUPS, 1), F32)
    nt = (((1,), (1,)), ((), ()))
    for k in range(cells):
        rows = slice(k * per, (k + 1) * per)
        value = lax.dot_general(press[rows, :], rate[0], nt, preferred_element_type=F32)
        value += lax.dot_general(change[rows, :], rate[1], nt, preferred_element_type=F32)
        part_send[k, 0:per, :] = value
        member = (group_ref[:, rows] == label).astype(F32)
        members += jnp.sum(member, axis=1, keepdims=True)
        total += jnp.dot(
            member, value, precision=lax.Precision.HIGHEST, preferred_element_type=F32
        )
    for k in range(cells):
        part_send[k, per : per + GROUPS, :] = total

    def part_copy(d):
        return pltpu.make_async_remote_copy(
            src_ref=part_send.at[lax.rem(c + d, cells)],
            dst_ref=part_recv.at[c],
            send_sem=part_ssem.at[d],
            recv_sem=part_rsem.at[d],
            device_id=cell_peer(d),
            device_id_type=MESH,
        )

    for d in range(1, cells):
        part_copy(d).start()
    part_recv[c] = part_send[c]

    @pl.loop(0, height // 8)
    def _(i):
        rows = pl.ds(pl.multiple_of(i * 8, 8), 8)
        field_out[rows, :] = u[STEPS % 2, rows, :]

    for d in range(1, cells):
        part_copy(d).wait_recv()
    summed = part_recv[0]
    for k in range(1, cells):
        summed = summed + part_recv[k]
    share = per // passes
    for k in range(passes):
        sum_send[k, 0:share, :] = summed[k * share : (k + 1) * share, :]
        sum_send[k, share : share + GROUPS, :] = summed[per : per + GROUPS, :]

    def sum_copy(d):
        return pltpu.make_async_remote_copy(
            src_ref=sum_send.at[lax.rem(p + d, passes)],
            dst_ref=sum_recv.at[p],
            send_sem=sum_ssem.at[d],
            recv_sem=sum_rsem.at[d],
            device_id=pass_peer(d),
            device_id_type=MESH,
        )

    def all_copy(d):
        return pltpu.make_async_remote_copy(
            src_ref=own,
            dst_ref=gathered.at[p],
            send_sem=all_ssem.at[d],
            recv_sem=all_rsem.at[d],
            device_id=pass_peer(d),
            device_id_type=MESH,
        )

    @pl.loop(1, passes)
    def _(d):
        sum_copy(d).start()

    sum_recv[p] = sum_send[p]

    @pl.loop(1, passes)
    def _(d):
        sum_copy(d).wait_recv()

    result = sum_recv[0]
    for k in range(1, passes):
        result = result + sum_recv[k]
    own[...] = result[0:share, :]

    @pl.loop(1, passes)
    def _(d):
        all_copy(d).start()

    gathered[p] = result[0:share, :]
    array_out[...] = result[share : share + GROUPS, :] / jnp.maximum(members, 1.0)

    @pl.loop(1, passes)
    def _(d):
        all_copy(d).wait_recv()

    acoustic_out[...] = gathered[...]

    @pl.loop(0, STEPS)
    def _(m):
        for way in range(2):
            row_copy(m, way).wait_send()
            col_copy(m, way).wait_send()

    for d in range(1, cells):
        part_copy(d).wait_send()

    @pl.loop(1, passes)
    def _(d):
        sum_copy(d).wait_send()
        all_copy(d).wait_send()


def on_device(
    passes,
    cells,
    flow_state,
    face_weights,
    forcing,
    lagged_planes,
    phase_lag,
    face_map,
    surface_record,
    face_radius,
    face_angle,
    face_axial,
    face_stagger,
    face_area,
    listeners,
    observer_group,
):
    height, width = flow_state.shape
    lags = lagged_planes.shape[1]
    observers = listeners.shape[1]
    times = surface_record.shape[1] + STEPS
    per = observers // cells
    share = per // passes
    slab = width // 128
    hist = -(-(lags + STEPS + 1) // 8) * 8
    vmem = pl.BlockSpec(memory_space=pltpu.VMEM)
    dma = pltpu.SemaphoreType.DMA
    field, acoustic, signal = pl.pallas_call(
        functools.partial(body, passes, cells),
        out_shape=(
            jax.ShapeDtypeStruct((height, width), F32),
            jax.ShapeDtypeStruct((passes, share, times), F32),
            jax.ShapeDtypeStruct((GROUPS, times), F32),
        ),
        in_specs=[pl.BlockSpec(memory_space=pltpu.SMEM)] + [vmem] * 13,
        out_specs=(vmem, vmem, vmem),
        scratch_shapes=[
            pltpu.VMEM((2, height, width), F32),
            pltpu.VMEM((height, width), F32),
            pltpu.VMEM((hist, width), F32),
            pltpu.VMEM((hist, width), F32),
            pltpu.VMEM((STEPS, 2, slab, 128), F32),
            pltpu.VMEM((STEPS, 2, slab, 128), F32),
            pltpu.VMEM((STEPS, 2, height // 128, 128), F32),
            pltpu.VMEM((STEPS, 2, height // 128, 128), F32),
            pltpu.VMEM((height, 128), F32),
            pltpu.VMEM((times, width), F32),
            pltpu.VMEM((2, times, width), BF16),
            pltpu.VMEM((6, slab, 128), F32),
            pltpu.VMEM((observers, width), BF16),
            pltpu.VMEM((observers, width), BF16),
            pltpu.VMEM((cells, per + GROUPS, times), F32),
            pltpu.VMEM((cells, per + GROUPS, times), F32),
            pltpu.VMEM((passes, share + GROUPS, times), F32),
            pltpu.VMEM((passes, share + GROUPS, times), F32),
            pltpu.VMEM((share, times), F32),
            pltpu.VMEM((passes, share, times), F32),
            dma((STEPS, 2)),
            dma((STEPS, 2)),
            dma((STEPS, 2)),
            dma((STEPS, 2)),
            dma((cells,)),
            dma((cells,)),
            dma((passes,)),
            dma((passes,)),
            dma((passes,)),
            dma((passes,)),
        ],
        compiler_params=pltpu.CompilerParams(
            collective_id=0, has_side_effects=True, vmem_limit_bytes=60000 * 1024
        ),
        name="march",
    )(
        phase_lag,
        flow_state,
        face_weights,
        forcing,
        lagged_planes,
        face_map,
        surface_record,
        face_radius,
        face_angle,
        face_axial,
        face_stagger,
        face_area,
        listeners,
        observer_group.reshape(1, observers),
    )
    return field, acoustic.reshape(per, times), signal


def solution(mesh):
    return jax.shard_map(
        functools.partial(on_device, mesh.shape["pass"], mesh.shape["cell"]),
        mesh=mesh,
        in_specs=(
            P("pass", "cell"),
            P(None, "pass", "cell"),
            P("pass", "cell"),
            P("pass", None, "cell"),
            P(),
            P("pass", "cell"),
            P("pass", None, "cell"),
            P(None, "cell"),
            P(None, "cell"),
            P(None, "cell"),
            P(None, "cell"),
            P(None, "cell"),
            P(),
            P(),
        ),
        out_specs=(P("pass", "cell"), P("cell", None), P()),
        check_vma=False,
    )
```

```python
import functools
import math

import jax
import jax.numpy as jnp
from jax import lax
from jax.experimental import pallas as pl
from jax.experimental.pallas import tpu as pltpu
from jax.sharding import PartitionSpec as P

STEPS = 8
GROUPS = 16
SOUND = 2.0
MESH = pl.DeviceIdType.MESH
F32 = jnp.float32
BF16 = jnp.bfloat16


def fold(row):
    width = row.shape[1]
    return jnp.concatenate([row[:, i : i + 128] for i in range(0, width, 128)], axis=0)


def unfold(slab):
    return jnp.concatenate([slab[i : i + 1, :] for i in range(slab.shape[0])], axis=1)


def iota(shape, dim):
    return lax.broadcasted_iota(jnp.int32, shape, dim)


def body(
    passes,
    cells,
    lag_ref,
    u_in,
    w_in,
    f_in,
    planes_ref,
    map_ref,
    record_ref,
    radius_ref,
    angle_ref,
    axial_ref,
    stagger_ref,
    area_ref,
    points_ref,
    group_ref,
    field_out,
    acoustic_out,
    array_out,
    ua,
    ub,
    w_ref,
    f_ref,
    keep,
    low_hist,
    up_hist,
    row_send,
    row_recv,
    col_send,
    col_recv,
    rim,
    surf,
    rate,
    faces,
    press,
    change,
    part_send,
    part_recv,
    sum_send,
    sum_recv,
    own,
    gathered,
    row_ssem,
    row_rsem,
    col_ssem,
    col_rsem,
    part_ssem,
    part_rsem,
    sum_ssem,
    sum_rsem,
    all_ssem,
    all_rsem,
    load_sem,
):
    p = lax.axis_index("pass")
    c = lax.axis_index("cell")
    height, width = u_in.shape
    half = lax.rem(p, 2)
    passage = lax.div(p, 2)
    count = passes // 2
    lags = planes_ref.shape[1]
    observers = points_ref.shape[1]
    records = record_ref.shape[1]
    times = records + STEPS

    def pass_peer(d):
        return (lax.rem(p + d, passes), c)

    def cell_peer(d):
        return (p, lax.rem(c + d, cells))

    loads = [
        pltpu.make_async_copy(a, b, load_sem.at[i])
        for i, (a, b) in enumerate(((u_in, ua), (w_in, w_ref), (f_in, f_ref)))
    ]
    for load in loads:
        load.start()
    barrier = pltpu.get_barrier_semaphore()
    for d in range(1, cells):
        pl.semaphore_signal(barrier, inc=1, device_id=cell_peer(d), device_id_type=MESH)

    @pl.loop(1, passes)
    def _(d):
        pl.semaphore_signal(barrier, inc=1, device_id=pass_peer(d), device_id_type=MESH)

    after_lag = lag_ref[lax.rem(passage + 1, count), 0]
    before_lag = lag_ref[lax.rem(passage + count - 1, count), 1]
    up_pick = jnp.where(half == 1, after_lag, 0)
    down_pick = jnp.where(half == 0, before_lag, 0)

    def row_copy(level, way):
        d = 1 if way == 0 else passes - 1
        return pltpu.make_async_remote_copy(
            src_ref=row_send.at[level, way],
            dst_ref=row_recv.at[level, way],
            send_sem=row_ssem.at[level, way],
            recv_sem=row_rsem.at[level, way],
            device_id=pass_peer(d),
            device_id_type=MESH,
        )

    def col_copy(level, way):
        d = 1 if way == 0 else cells - 1
        return pltpu.make_async_remote_copy(
            src_ref=col_send.at[level, way],
            dst_ref=col_recv.at[level, way],
            send_sem=col_ssem.at[level, way],
            recv_sem=col_rsem.at[level, way],
            device_id=cell_peer(d),
            device_id_type=MESH,
        )

    def send_rows(level):
        row_send[level, 0] = fold(up_hist[pl.ds(lags + level - up_pick, 1), :])
        row_send[level, 1] = fold(low_hist[pl.ds(lags + level - down_pick, 1), :])
        row_copy(level, 0).start()
        row_copy(level, 1).start()

    lane = iota((128, 128), 1)
    sub = iota((128, 128), 0)

    def send_cols(level, first, last):
        for k in range(height // 128):
            rows = pl.ds(k * 128, 128)
            both = jnp.where(lane == 127, last(rows), first(rows)).T
            col_send[level, 1, k : k + 1, :] = both[0:1, :]
            col_send[level, 0, k : k + 1, :] = both[127:128, :]
        col_copy(level, 0).start()
        col_copy(level, 1).start()

    for j in range(lags):
        low_hist[lags - 1 - j : lags - j, :] = planes_ref[0, j : j + 1, :]
        up_hist[lags - 1 - j : lags - j, :] = planes_ref[0, j : j + 1, :]
    loads[0].wait()
    low_hist[lags : lags + 1, :] = ua[0:1, :]
    up_hist[lags : lags + 1, :] = ua[height - 1 : height, :]

    pl.semaphore_wait(barrier, cells - 1 + passes - 1)
    send_rows(0)
    send_cols(0, lambda rows: ua[rows, 0:128], lambda rows: ua[rows, width - 128 : width])

    local_map = fold(map_ref[...]) - c * width
    map_row = lax.div(local_map, 128)
    map_lane = lax.rem(local_map, 128)

    surf[0:records, :] = record_ref[0].astype(F32)
    surf[records:times, :] = jnp.zeros((times - records, width), F32)
    theta = passage.astype(F32) * (2.0 * math.pi / count)
    scale = 64.0 / math.sqrt(width * cells * passes)
    mine = pl.ds(half, 1)
    phase = theta + fold(angle_ref[mine, :])
    cos_phase = jnp.cos(phase)
    sin_phase = jnp.sin(phase)
    stagger = fold(stagger_ref[mine, :])
    cos_stagger = jnp.cos(stagger)
    sin_stagger = jnp.sin(stagger)
    radius = fold(radius_ref[mine, :])
    weight = fold(area_ref[mine, :]) * (scale / (4.0 * math.pi))
    faces[0] = radius * cos_phase
    faces[1] = radius * sin_phase
    faces[2] = fold(axial_ref[mine, :])
    faces[3] = -cos_stagger * sin_phase * weight
    faces[4] = cos_stagger * cos_phase * weight
    faces[5] = sin_stagger * weight

    def rates(start):
        for j in range(width // 128):
            cols = slice(j * 128, (j + 1) * 128)
            base = max(start - 8, 0)
            v = surf[base:times, cols]
            rows = times - base
            tt = iota(v.shape, 0) + base
            nxt = pltpu.roll(v, rows - 1, 0)
            prv = pltpu.roll(v, 1, 0)
            r = jnp.where(
                tt == 0, nxt - v, jnp.where(tt == times - 1, v - prv, (nxt - prv) * 0.5)
            )
            rate[0, start:times, cols] = v[start - base :].astype(BF16)
            rate[1, start:times, cols] = r[start - base :].astype(BF16)

    rates(0)
    loads[1].wait()

    @pl.loop(0, height // 8, unroll=4)
    def _(i):
        rows = pl.ds(pl.multiple_of(i * 8, 8), 8)
        keep[rows, :] = (
            1.0 - w_ref[0, rows, :] - w_ref[1, rows, :] - w_ref[2, rows, :] - w_ref[3, rows, :]
        )

    loads[2].wait()
    lane8 = iota((8, 128), 1)
    sub8 = iota((8, width), 0)

    def block(dst, start, now, before, after):
        rows = pl.ds(start, 8)
        edge = rim[rows, :]
        below = pltpu.roll(jnp.where(sub8 == 7, before, now), 1, 0)
        above = pltpu.roll(jnp.where(sub8 == 0, after, now), 7, 0)
        left = pltpu.roll(now, 1, 1)
        right = pltpu.roll(now, width - 1, 1)
        left = jnp.concatenate(
            [jnp.where(lane8 == 0, edge, left[:, :128]), left[:, 128:]], axis=1
        )
        right = jnp.concatenate(
            [right[:, : width - 128], jnp.where(lane8 == 127, edge, right[:, width - 128 :])],
            axis=1,
        )
        value = (
            keep[rows, :] * now
            + w_ref[0, rows, :] * below
            + w_ref[1, rows, :] * above
            + w_ref[2, rows, :] * left
            + w_ref[3, rows, :] * right
            + f_ref[rows, :]
        )
        dst[rows, :] = value
        return value

    chunk = observers // STEPS
    inner = height // 8 - 2
    group = max(k for k in range(1, 7) if inner % k == 0)

    def kernels(step):
        @pl.loop(0, chunk // 128)
        def _(k):
            base = pl.multiple_of(step * chunk + k * 128, 128)
            xyz = [
                jnp.broadcast_to(points_ref[i : i + 1, pl.ds(base, 128)], (128, 128)).T
                for i in range(3)
            ]
            for j in range(width // 128):
                row = [faces[i, j : j + 1, :] for i in range(6)]
                for s in range(0, 128, 32):
                    dx = xyz[0][s : s + 32] - row[0]
                    dy = xyz[1][s : s + 32] - row[1]
                    dz = xyz[2][s : s + 32] - row[2]
                    inv = lax.rsqrt(dx * dx + dy * dy + dz * dz)
                    dot = row[3] * dx + row[4] * dy + row[5] * dz
                    q = dot * (inv * inv)
                    at = (pl.ds(base + s, 32), pl.ds(j * 128, 128))
                    press[at] = (q * inv).astype(BF16)
                    change[at] = (q * (1.0 / SOUND)).astype(BF16)

    def advance(m, src, dst):
        for way in range(2):
            col_copy(m, way).wait_recv()
        col_l = jnp.where(c > 0, col_recv[m, 0], 0.0)
        col_r = jnp.where(c < cells - 1, col_recv[m, 1], 0.0)
        for k in range(height // 128):
            rim[k * 128 : (k + 1) * 128, :] = jnp.where(
                sub < 64, col_l[k : k + 1, :], col_r[k : k + 1, :]
            ).T
        for way in range(2):
            row_copy(m, way).wait_recv()
        raw_low = row_recv[m, 0]
        raw_high = row_recv[m, 1]
        raw = jnp.where(half == 0, raw_low, raw_high)
        mapped = jnp.zeros_like(raw)
        for s in range(width // 128):
            picked = jnp.take_along_axis(
                jnp.broadcast_to(raw[s : s + 1, :], raw.shape),
                map_lane,
                axis=1,
                mode="promise_in_bounds",
            )
            mapped = jnp.where(map_row == s, picked, mapped)
        ghost_low = unfold(jnp.where(half == 0, mapped, raw_low))
        ghost_high = unfold(jnp.where(half == 1, mapped, raw_high))
        first = block(dst, 0, src[0:8, :], ghost_low, src[8:16, :])
        last = block(
            dst, height - 8, src[height - 8 :, :], src[height - 16 : height - 8, :], ghost_high
        )
        low_hist[pl.ds(lags + m + 1, 1), :] = first[0:1, :]
        up_hist[pl.ds(lags + m + 1, 1), :] = last[7:8, :]

        @pl.when(m < STEPS - 1)
        def _():
            send_rows(m + 1)

        @pl.loop(0, inner // group)
        def _(i):
            start = pl.multiple_of(i * (8 * group), 8)
            tiles = [src[pl.ds(pl.multiple_of(start + 8 * k, 8), 8), :] for k in range(group + 2)]
            for k in range(1, group + 1):
                block(
                    dst,
                    pl.multiple_of(start + 8 * k, 8),
                    tiles[k],
                    tiles[k - 1],
                    tiles[k + 1],
                )

        @pl.when(m < STEPS - 1)
        def _():
            send_cols(
                m + 1,
                lambda rows: dst[rows, 0:128],
                lambda rows: dst[rows, width - 128 : width],
            )

        side = dst[height // 2 : height // 2 + 1, :]
        surf[pl.ds(records + m, 1), :] = side.astype(BF16).astype(F32)
        kernels(m)

    @pl.loop(0, STEPS // 2)
    def _(k):
        advance(2 * k, ua, ub)
        advance(2 * k + 1, ub, ua)


    late = (records - 1) // 16 * 16
    rates(late)
    store = pltpu.make_async_copy(ua, field_out, load_sem.at[0])
    store.start()
    per = observers // cells
    total = jnp.zeros((GROUPS, times), F32)
    label = iota((GROUPS, per), 0)
    members = jnp.zeros((GROUPS, 1), F32)
    nt = (((1,), (1,)), ((), ()))
    for k in range(cells):
        rows = slice(k * per, (k + 1) * per)
        value = lax.dot_general(press[rows, :], rate[0], nt, preferred_element_type=F32)
        value += lax.dot_general(change[rows, :], rate[1], nt, preferred_element_type=F32)
        part_send[k, 0:per, :] = value
        member = (group_ref[:, rows] == label).astype(F32)
        members += jnp.sum(member, axis=1, keepdims=True)
        total += jnp.dot(
            member, value, precision=lax.Precision.HIGHEST, preferred_element_type=F32
        )
    for k in range(cells):
        part_send[k, per : per + GROUPS, :] = total

    def part_copy(d):
        return pltpu.make_async_remote_copy(
            src_ref=part_send.at[lax.rem(c + d, cells)],
            dst_ref=part_recv.at[c],
            send_sem=part_ssem.at[d],
            recv_sem=part_rsem.at[d],
            device_id=cell_peer(d),
            device_id_type=MESH,
        )

    for d in range(1, cells):
        part_copy(d).start()
    part_recv[c] = part_send[c]

    for d in range(1, cells):
        part_copy(d).wait_recv()
    summed = part_recv[0]
    for k in range(1, cells):
        summed = summed + part_recv[k]
    share = per // passes
    for k in range(passes):
        sum_send[k, 0:share, :] = summed[k * share : (k + 1) * share, :]
        sum_send[k, share : share + GROUPS, :] = summed[per : per + GROUPS, :]

    def sum_copy(d):
        return pltpu.make_async_remote_copy(
            src_ref=sum_send.at[lax.rem(p + d, passes)],
            dst_ref=sum_recv.at[p],
            send_sem=sum_ssem.at[d],
            recv_sem=sum_rsem.at[d],
            device_id=pass_peer(d),
            device_id_type=MESH,
        )

    def all_copy(d):
        return pltpu.make_async_remote_copy(
            src_ref=own,
            dst_ref=gathered.at[p],
            send_sem=all_ssem.at[d],
            recv_sem=all_rsem.at[d],
            device_id=pass_peer(d),
            device_id_type=MESH,
        )

    @pl.loop(1, passes)
    def _(d):
        sum_copy(d).start()

    sum_recv[p] = sum_send[p]

    @pl.loop(1, passes)
    def _(d):
        sum_copy(d).wait_recv()

    result = sum_recv[0]
    for k in range(1, passes):
        result = result + sum_recv[k]
    own[...] = result[0:share, :]

    @pl.loop(1, passes)
    def _(d):
        all_copy(d).start()

    gathered[p] = result[0:share, :]
    array_out[...] = result[share : share + GROUPS, :] / jnp.maximum(members, 1.0)

    @pl.loop(1, passes)
    def _(d):
        all_copy(d).wait_recv()

    acoustic_out[...] = gathered[...]
    store.wait()

    @pl.loop(0, STEPS)
    def _(m):
        for way in range(2):
            row_copy(m, way).wait_send()
            col_copy(m, way).wait_send()

    for d in range(1, cells):
        part_copy(d).wait_send()

    @pl.loop(1, passes)
    def _(d):
        sum_copy(d).wait_send()
        all_copy(d).wait_send()


def deliver_body(pieces, *refs):
    sources, targets = refs[:3], refs[3:6]
    held = refs[6:9]
    read_sem, write_sem = refs[9:]
    moves = []
    for k in range(3):
        rows = sources[k].shape[0]
        parts = pieces if k == 0 else 1
        for i in range(parts):
            at = pl.ds(i * (rows // parts), rows // parts)
            n = len(moves)
            moves.append(
                (
                    pltpu.make_async_copy(sources[k].at[at], held[k].at[at], read_sem.at[n]),
                    pltpu.make_async_copy(held[k].at[at], targets[k].at[at], write_sem.at[n]),
                )
            )
    for read, _ in moves:
        read.start()
    for read, write in moves:
        read.wait()
        write.start()
    for _, write in moves:
        write.wait()


def deliver(*arrays):
    hbm = pl.BlockSpec(memory_space=pl.ANY)
    pieces = 4
    return pl.pallas_call(
        functools.partial(deliver_body, pieces),
        out_shape=tuple(jax.ShapeDtypeStruct(a.shape, a.dtype) for a in arrays),
        in_specs=[hbm] * 3,
        out_specs=(hbm,) * 3,
        scratch_shapes=[pltpu.VMEM(a.shape, a.dtype) for a in arrays]
        + [pltpu.SemaphoreType.DMA((pieces + 2,))] * 2,
        name="deliver",
    )(*arrays)


def on_device(
    passes,
    cells,
    flow_state,
    face_weights,
    forcing,
    lagged_planes,
    phase_lag,
    face_map,
    surface_record,
    face_radius,
    face_angle,
    face_axial,
    face_stagger,
    face_area,
    listeners,
    observer_group,
):
    height, width = flow_state.shape
    lags = lagged_planes.shape[1]
    observers = listeners.shape[1]
    times = surface_record.shape[1] + STEPS
    per = observers // cells
    share = per // passes
    slab = width // 128
    hist = -(-(lags + STEPS + 1) // 8) * 8
    vmem = pl.BlockSpec(memory_space=pltpu.VMEM)
    hbm = pl.BlockSpec(memory_space=pl.ANY)
    dma = pltpu.SemaphoreType.DMA
    field, acoustic, signal = pl.pallas_call(
        functools.partial(body, passes, cells),
        out_shape=(
            jax.ShapeDtypeStruct((height, width), F32),
            jax.ShapeDtypeStruct((passes, share, times), F32),
            jax.ShapeDtypeStruct((GROUPS, times), F32),
        ),
        in_specs=[pl.BlockSpec(memory_space=pltpu.SMEM)] + [hbm] * 3 + [vmem] * 10,
        out_specs=(hbm, vmem, vmem),
        scratch_shapes=[
            pltpu.VMEM((height, width), F32),
            pltpu.VMEM((height, width), F32),
            pltpu.VMEM((4, height, width), F32),
            pltpu.VMEM((height, width), F32),
            pltpu.VMEM((height, width), F32),
            pltpu.VMEM((hist, width), F32),
            pltpu.VMEM((hist, width), F32),
            pltpu.VMEM((STEPS, 2, slab, 128), F32),
            pltpu.VMEM((STEPS, 2, slab, 128), F32),
            pltpu.VMEM((STEPS, 2, height // 128, 128), F32),
            pltpu.VMEM((STEPS, 2, height // 128, 128), F32),
            pltpu.VMEM((height, 128), F32),
            pltpu.VMEM((times, width), F32),
            pltpu.VMEM((2, times, width), BF16),
            pltpu.VMEM((6, slab, 128), F32),
            pltpu.VMEM((observers, width), BF16),
            pltpu.VMEM((observers, width), BF16),
            pltpu.VMEM((cells, per + GROUPS, times), F32),
            pltpu.VMEM((cells, per + GROUPS, times), F32),
            pltpu.VMEM((passes, share + GROUPS, times), F32),
            pltpu.VMEM((passes, share + GROUPS, times), F32),
            pltpu.VMEM((share, times), F32),
            pltpu.VMEM((passes, share, times), F32),
            dma((STEPS, 2)),
            dma((STEPS, 2)),
            dma((STEPS, 2)),
            dma((STEPS, 2)),
            dma((cells,)),
            dma((cells,)),
            dma((passes,)),
            dma((passes,)),
            dma((passes,)),
            dma((passes,)),
            dma((3,)),
        ],
        compiler_params=pltpu.CompilerParams(
            collective_id=0, has_side_effects=True, vmem_limit_bytes=60000 * 1024
        ),
        name="march",
    )(
        phase_lag,
        flow_state,
        face_weights,
        forcing,
        lagged_planes,
        face_map,
        surface_record,
        face_radius,
        face_angle,
        face_axial,
        face_stagger,
        face_area,
        listeners,
        observer_group.reshape(1, observers),
    )
    return deliver(field, acoustic.reshape(per, times), signal)


def solution(mesh):
    return jax.shard_map(
        functools.partial(on_device, mesh.shape["pass"], mesh.shape["cell"]),
        mesh=mesh,
        in_specs=(
            P("pass", "cell"),
            P(None, "pass", "cell"),
            P("pass", "cell"),
            P("pass", None, "cell"),
            P(),
            P("pass", "cell"),
            P("pass", None, "cell"),
            P(None, "cell"),
            P(None, "cell"),
            P(None, "cell"),
            P(None, "cell"),
            P(None, "cell"),
            P(),
            P(),
        ),
        out_specs=(P("pass", "cell"), P("cell", None), P()),
        check_vma=False,
    )
```

```python
import functools
import math

import jax
import jax.numpy as jnp
from jax import lax
from jax.experimental import pallas as pl
from jax.experimental.pallas import tpu as pltpu
from jax.sharding import PartitionSpec as P

STEPS = 8
GROUPS = 16
SOUND = 2.0
MESH = pl.DeviceIdType.MESH
F32 = jnp.float32
BF16 = jnp.bfloat16


def fold(row):
    width = row.shape[1]
    return jnp.concatenate([row[:, i : i + 128] for i in range(0, width, 128)], axis=0)


def unfold(slab):
    return jnp.concatenate([slab[i : i + 1, :] for i in range(slab.shape[0])], axis=1)


def iota(shape, dim):
    return lax.broadcasted_iota(jnp.int32, shape, dim)


def body(
    passes,
    cells,
    lag_ref,
    u_in,
    w_in,
    f_in,
    planes_ref,
    map_ref,
    record_ref,
    radius_ref,
    angle_ref,
    axial_ref,
    stagger_ref,
    area_ref,
    points_ref,
    group_ref,
    field_out,
    acoustic_out,
    array_out,
    ua,
    ub,
    w_ref,
    f_ref,
    keep,
    low_hist,
    up_hist,
    row_send,
    row_recv,
    col_send,
    col_recv,
    rim,
    surf,
    rate,
    faces,
    press,
    change,
    part_send,
    part_recv,
    sum_send,
    sum_recv,
    own,
    gathered,
    row_ssem,
    row_rsem,
    col_ssem,
    col_rsem,
    part_ssem,
    part_rsem,
    sum_ssem,
    sum_rsem,
    all_ssem,
    all_rsem,
    load_sem,
):
    p = lax.axis_index("pass")
    c = lax.axis_index("cell")
    height, width = u_in.shape
    half = lax.rem(p, 2)
    passage = lax.div(p, 2)
    count = passes // 2
    lags = planes_ref.shape[1]
    observers = points_ref.shape[1]
    records = record_ref.shape[1]
    times = records + STEPS

    def pass_peer(d):
        return (lax.rem(p + d, passes), c)

    def cell_peer(d):
        return (p, lax.rem(c + d, cells))

    loads = [
        pltpu.make_async_copy(a, b, load_sem.at[i])
        for i, (a, b) in enumerate(((u_in, ua), (w_in, w_ref), (f_in, f_ref)))
    ]
    for load in loads:
        load.start()
    barrier = pltpu.get_barrier_semaphore()
    for d in range(1, cells):
        pl.semaphore_signal(barrier, inc=1, device_id=cell_peer(d), device_id_type=MESH)

    @pl.loop(1, passes)
    def _(d):
        pl.semaphore_signal(barrier, inc=1, device_id=pass_peer(d), device_id_type=MESH)

    after_lag = lag_ref[0, lax.rem(passage + 1, count)]
    before_lag = lag_ref[1, lax.rem(passage + count - 1, count)]
    up_pick = jnp.where(half == 1, after_lag, 0)
    down_pick = jnp.where(half == 0, before_lag, 0)

    def row_copy(level, way):
        d = 1 if way == 0 else passes - 1
        return pltpu.make_async_remote_copy(
            src_ref=row_send.at[level, way],
            dst_ref=row_recv.at[level, way],
            send_sem=row_ssem.at[level, way],
            recv_sem=row_rsem.at[level, way],
            device_id=pass_peer(d),
            device_id_type=MESH,
        )

    def col_copy(level, way):
        d = 1 if way == 0 else cells - 1
        return pltpu.make_async_remote_copy(
            src_ref=col_send.at[level, way],
            dst_ref=col_recv.at[level, way],
            send_sem=col_ssem.at[level, way],
            recv_sem=col_rsem.at[level, way],
            device_id=cell_peer(d),
            device_id_type=MESH,
        )

    def send_rows(level):
        row_send[level, 0] = fold(up_hist[pl.ds(lags + level - up_pick, 1), :])
        row_send[level, 1] = fold(low_hist[pl.ds(lags + level - down_pick, 1), :])
        row_copy(level, 0).start()
        row_copy(level, 1).start()

    lane = iota((128, 128), 1)
    sub = iota((128, 128), 0)

    def send_cols(level, first, last):
        for k in range(height // 128):
            rows = pl.ds(k * 128, 128)
            both = jnp.where(lane == 127, last(rows), first(rows)).T
            col_send[level, 1, k : k + 1, :] = both[0:1, :]
            col_send[level, 0, k : k + 1, :] = both[127:128, :]
        col_copy(level, 0).start()
        col_copy(level, 1).start()

    for j in range(lags):
        low_hist[lags - 1 - j : lags - j, :] = planes_ref[0, j : j + 1, :]
        up_hist[lags - 1 - j : lags - j, :] = planes_ref[0, j : j + 1, :]
    loads[0].wait()
    low_hist[lags : lags + 1, :] = ua[0:1, :]
    up_hist[lags : lags + 1, :] = ua[height - 1 : height, :]

    pl.semaphore_wait(barrier, cells - 1 + passes - 1)
    send_rows(0)
    send_cols(0, lambda rows: ua[rows, 0:128], lambda rows: ua[rows, width - 128 : width])

    local_map = fold(map_ref[...]) - c * width
    map_row = lax.div(local_map, 128)
    map_lane = lax.rem(local_map, 128)

    surf[0:records, :] = record_ref[0].astype(F32)
    surf[records:times, :] = jnp.zeros((times - records, width), F32)
    theta = passage.astype(F32) * (2.0 * math.pi / count)
    scale = 64.0 / math.sqrt(width * cells * passes)
    mine = pl.ds(half, 1)
    phase = theta + fold(angle_ref[mine, :])
    cos_phase = jnp.cos(phase)
    sin_phase = jnp.sin(phase)
    stagger = fold(stagger_ref[mine, :])
    cos_stagger = jnp.cos(stagger)
    sin_stagger = jnp.sin(stagger)
    radius = fold(radius_ref[mine, :])
    weight = fold(area_ref[mine, :]) * (scale / (4.0 * math.pi))
    faces[0] = radius * cos_phase
    faces[1] = radius * sin_phase
    faces[2] = fold(axial_ref[mine, :])
    faces[3] = -cos_stagger * sin_phase * weight
    faces[4] = cos_stagger * cos_phase * weight
    faces[5] = sin_stagger * weight

    def rates(start):
        for j in range(width // 128):
            cols = slice(j * 128, (j + 1) * 128)
            base = max(start - 8, 0)
            v = surf[base:times, cols]
            rows = times - base
            tt = iota(v.shape, 0) + base
            nxt = pltpu.roll(v, rows - 1, 0)
            prv = pltpu.roll(v, 1, 0)
            r = jnp.where(
                tt == 0, nxt - v, jnp.where(tt == times - 1, v - prv, (nxt - prv) * 0.5)
            )
            rate[0, start:times, cols] = v[start - base :].astype(BF16)
            rate[1, start:times, cols] = r[start - base :].astype(BF16)

    rates(0)
    loads[1].wait()

    @pl.loop(0, height // 8, unroll=4)
    def _(i):
        rows = pl.ds(pl.multiple_of(i * 8, 8), 8)
        keep[rows, :] = (
            1.0 - w_ref[0, rows, :] - w_ref[1, rows, :] - w_ref[2, rows, :] - w_ref[3, rows, :]
        )

    loads[2].wait()
    lane8 = iota((8, 128), 1)
    sub8 = iota((8, width), 0)

    def block(dst, start, now, before, after):
        rows = pl.ds(start, 8)
        edge = rim[rows, :]
        below = pltpu.roll(jnp.where(sub8 == 7, before, now), 1, 0)
        above = pltpu.roll(jnp.where(sub8 == 0, after, now), 7, 0)
        left = pltpu.roll(now, 1, 1)
        right = pltpu.roll(now, width - 1, 1)
        left = jnp.concatenate(
            [jnp.where(lane8 == 0, edge, left[:, :128]), left[:, 128:]], axis=1
        )
        right = jnp.concatenate(
            [right[:, : width - 128], jnp.where(lane8 == 127, edge, right[:, width - 128 :])],
            axis=1,
        )
        value = (
            keep[rows, :] * now
            + w_ref[0, rows, :] * below
            + w_ref[1, rows, :] * above
            + w_ref[2, rows, :] * left
            + w_ref[3, rows, :] * right
            + f_ref[rows, :]
        )
        dst[rows, :] = value
        return value

    chunk = observers // STEPS
    inner = height // 8 - 2
    group = max(k for k in range(1, 7) if inner % k == 0)

    def kernels(step):
        @pl.loop(0, chunk // 128)
        def _(k):
            base = pl.multiple_of(step * chunk + k * 128, 128)
            xyz = [
                jnp.broadcast_to(points_ref[i : i + 1, pl.ds(base, 128)], (128, 128)).T
                for i in range(3)
            ]
            for j in range(width // 128):
                row = [faces[i, j : j + 1, :] for i in range(6)]
                for s in range(0, 128, 32):
                    dx = xyz[0][s : s + 32] - row[0]
                    dy = xyz[1][s : s + 32] - row[1]
                    dz = xyz[2][s : s + 32] - row[2]
                    inv = lax.rsqrt(dx * dx + dy * dy + dz * dz)
                    dot = row[3] * dx + row[4] * dy + row[5] * dz
                    q = dot * (inv * inv)
                    at = (pl.ds(base + s, 32), pl.ds(j * 128, 128))
                    press[at] = (q * inv).astype(BF16)
                    change[at] = (q * (1.0 / SOUND)).astype(BF16)

    def advance(m, src, dst):
        for way in range(2):
            col_copy(m, way).wait_recv()
        col_l = jnp.where(c > 0, col_recv[m, 0], 0.0)
        col_r = jnp.where(c < cells - 1, col_recv[m, 1], 0.0)
        for k in range(height // 128):
            rim[k * 128 : (k + 1) * 128, :] = jnp.where(
                sub < 64, col_l[k : k + 1, :], col_r[k : k + 1, :]
            ).T
        for way in range(2):
            row_copy(m, way).wait_recv()
        raw_low = row_recv[m, 0]
        raw_high = row_recv[m, 1]
        raw = jnp.where(half == 0, raw_low, raw_high)
        mapped = jnp.zeros_like(raw)
        for s in range(width // 128):
            picked = jnp.take_along_axis(
                jnp.broadcast_to(raw[s : s + 1, :], raw.shape),
                map_lane,
                axis=1,
                mode="promise_in_bounds",
            )
            mapped = jnp.where(map_row == s, picked, mapped)
        ghost_low = unfold(jnp.where(half == 0, mapped, raw_low))
        ghost_high = unfold(jnp.where(half == 1, mapped, raw_high))
        first = block(dst, 0, src[0:8, :], ghost_low, src[8:16, :])
        last = block(
            dst, height - 8, src[height - 8 :, :], src[height - 16 : height - 8, :], ghost_high
        )
        low_hist[pl.ds(lags + m + 1, 1), :] = first[0:1, :]
        up_hist[pl.ds(lags + m + 1, 1), :] = last[7:8, :]

        @pl.when(m < STEPS - 1)
        def _():
            send_rows(m + 1)

        @pl.loop(0, inner // group)
        def _(i):
            start = pl.multiple_of(i * (8 * group), 8)
            tiles = [src[pl.ds(pl.multiple_of(start + 8 * k, 8), 8), :] for k in range(group + 2)]
            for k in range(1, group + 1):
                block(
                    dst,
                    pl.multiple_of(start + 8 * k, 8),
                    tiles[k],
                    tiles[k - 1],
                    tiles[k + 1],
                )

        @pl.when(m < STEPS - 1)
        def _():
            send_cols(
                m + 1,
                lambda rows: dst[rows, 0:128],
                lambda rows: dst[rows, width - 128 : width],
            )

        side = dst[height // 2 : height // 2 + 1, :]
        surf[pl.ds(records + m, 1), :] = side.astype(BF16).astype(F32)
        kernels(m)

    @pl.loop(0, STEPS // 2)
    def _(k):
        advance(2 * k, ua, ub)
        advance(2 * k + 1, ub, ua)


    late = (records - 1) // 16 * 16
    rates(late)
    store = pltpu.make_async_copy(ua, field_out, load_sem.at[0])
    store.start()
    per = observers // cells
    total = jnp.zeros((GROUPS, times), F32)
    label = iota((GROUPS, per), 0)
    members = jnp.zeros((GROUPS, 1), F32)
    nt = (((1,), (1,)), ((), ()))
    for k in range(cells):
        rows = slice(k * per, (k + 1) * per)
        value = lax.dot_general(press[rows, :], rate[0], nt, preferred_element_type=F32)
        value += lax.dot_general(change[rows, :], rate[1], nt, preferred_element_type=F32)
        part_send[k, 0:per, :] = value
        member = (group_ref[:, rows] == label).astype(F32)
        members += jnp.sum(member, axis=1, keepdims=True)
        total += jnp.dot(
            member, value, precision=lax.Precision.HIGHEST, preferred_element_type=F32
        )
    for k in range(cells):
        part_send[k, per : per + GROUPS, :] = total

    def part_copy(d):
        return pltpu.make_async_remote_copy(
            src_ref=part_send.at[lax.rem(c + d, cells)],
            dst_ref=part_recv.at[c],
            send_sem=part_ssem.at[d],
            recv_sem=part_rsem.at[d],
            device_id=cell_peer(d),
            device_id_type=MESH,
        )

    for d in range(1, cells):
        part_copy(d).start()
    part_recv[c] = part_send[c]

    for d in range(1, cells):
        part_copy(d).wait_recv()
    summed = part_recv[0]
    for k in range(1, cells):
        summed = summed + part_recv[k]
    share = per // passes
    for k in range(passes):
        sum_send[k, 0:share, :] = summed[k * share : (k + 1) * share, :]
        sum_send[k, share : share + GROUPS, :] = summed[per : per + GROUPS, :]

    def sum_copy(d):
        return pltpu.make_async_remote_copy(
            src_ref=sum_send.at[lax.rem(p + d, passes)],
            dst_ref=sum_recv.at[p],
            send_sem=sum_ssem.at[d],
            recv_sem=sum_rsem.at[d],
            device_id=pass_peer(d),
            device_id_type=MESH,
        )

    def all_copy(d):
        return pltpu.make_async_remote_copy(
            src_ref=own,
            dst_ref=gathered.at[p],
            send_sem=all_ssem.at[d],
            recv_sem=all_rsem.at[d],
            device_id=pass_peer(d),
            device_id_type=MESH,
        )

    @pl.loop(1, passes)
    def _(d):
        sum_copy(d).start()

    sum_recv[p] = sum_send[p]

    @pl.loop(1, passes)
    def _(d):
        sum_copy(d).wait_recv()

    result = sum_recv[0]
    for k in range(1, passes):
        result = result + sum_recv[k]
    own[...] = result[0:share, :]

    @pl.loop(1, passes)
    def _(d):
        all_copy(d).start()

    gathered[p] = result[0:share, :]
    array_out[...] = result[share : share + GROUPS, :] / jnp.maximum(members, 1.0)

    @pl.loop(1, passes)
    def _(d):
        all_copy(d).wait_recv()

    acoustic_out[...] = gathered[...]
    store.wait()

    @pl.loop(0, STEPS)
    def _(m):
        for way in range(2):
            row_copy(m, way).wait_send()
            col_copy(m, way).wait_send()

    for d in range(1, cells):
        part_copy(d).wait_send()

    @pl.loop(1, passes)
    def _(d):
        sum_copy(d).wait_send()
        all_copy(d).wait_send()


def deliver_body(pieces, *refs):
    sources, targets = refs[:3], refs[3:6]
    held = refs[6:9]
    read_sem, write_sem = refs[9:]
    moves = []
    for k in range(3):
        rows = sources[k].shape[0]
        parts = pieces if k == 0 else 1
        for i in range(parts):
            at = pl.ds(i * (rows // parts), rows // parts)
            n = len(moves)
            moves.append(
                (
                    pltpu.make_async_copy(sources[k].at[at], held[k].at[at], read_sem.at[n]),
                    pltpu.make_async_copy(held[k].at[at], targets[k].at[at], write_sem.at[n]),
                )
            )
    for read, _ in moves:
        read.start()
    for read, write in moves:
        read.wait()
        write.start()
    for _, write in moves:
        write.wait()


def deliver(*arrays):
    hbm = pl.BlockSpec(memory_space=pl.ANY)
    pieces = 4
    return pl.pallas_call(
        functools.partial(deliver_body, pieces),
        out_shape=tuple(jax.ShapeDtypeStruct(a.shape, a.dtype) for a in arrays),
        in_specs=[hbm] * 3,
        out_specs=(hbm,) * 3,
        scratch_shapes=[pltpu.VMEM(a.shape, a.dtype) for a in arrays]
        + [pltpu.SemaphoreType.DMA((pieces + 2,))] * 2,
        name="deliver",
    )(*arrays)


def on_device(
    passes,
    cells,
    flow_state,
    face_weights,
    forcing,
    lagged_planes,
    phase_lag,
    face_map,
    surface_record,
    face_radius,
    face_angle,
    face_axial,
    face_stagger,
    face_area,
    listeners,
    observer_group,
):
    height, width = flow_state.shape
    lags = lagged_planes.shape[1]
    observers = listeners.shape[1]
    times = surface_record.shape[1] + STEPS
    per = observers // cells
    share = per // passes
    slab = width // 128
    hist = -(-(lags + STEPS + 1) // 8) * 8
    vmem = pl.BlockSpec(memory_space=pltpu.VMEM)
    hbm = pl.BlockSpec(memory_space=pl.ANY)
    dma = pltpu.SemaphoreType.DMA
    field, acoustic, signal = pl.pallas_call(
        functools.partial(body, passes, cells),
        out_shape=(
            jax.ShapeDtypeStruct((height, width), F32),
            jax.ShapeDtypeStruct((passes, share, times), F32),
            jax.ShapeDtypeStruct((GROUPS, times), F32),
        ),
        in_specs=[pl.BlockSpec(memory_space=pltpu.SMEM)] + [hbm] * 3 + [vmem] * 10,
        out_specs=(hbm, vmem, vmem),
        scratch_shapes=[
            pltpu.VMEM((height, width), F32),
            pltpu.VMEM((height, width), F32),
            pltpu.VMEM((4, height, width), F32),
            pltpu.VMEM((height, width), F32),
            pltpu.VMEM((height, width), F32),
            pltpu.VMEM((hist, width), F32),
            pltpu.VMEM((hist, width), F32),
            pltpu.VMEM((STEPS, 2, slab, 128), F32),
            pltpu.VMEM((STEPS, 2, slab, 128), F32),
            pltpu.VMEM((STEPS, 2, height // 128, 128), F32),
            pltpu.VMEM((STEPS, 2, height // 128, 128), F32),
            pltpu.VMEM((height, 128), F32),
            pltpu.VMEM((times, width), F32),
            pltpu.VMEM((2, times, width), BF16),
            pltpu.VMEM((6, slab, 128), F32),
            pltpu.VMEM((observers, width), BF16),
            pltpu.VMEM((observers, width), BF16),
            pltpu.VMEM((cells, per + GROUPS, times), F32),
            pltpu.VMEM((cells, per + GROUPS, times), F32),
            pltpu.VMEM((passes, share + GROUPS, times), F32),
            pltpu.VMEM((passes, share + GROUPS, times), F32),
            pltpu.VMEM((share, times), F32),
            pltpu.VMEM((passes, share, times), F32),
            dma((STEPS, 2)),
            dma((STEPS, 2)),
            dma((STEPS, 2)),
            dma((STEPS, 2)),
            dma((cells,)),
            dma((cells,)),
            dma((passes,)),
            dma((passes,)),
            dma((passes,)),
            dma((passes,)),
            dma((3,)),
        ],
        compiler_params=pltpu.CompilerParams(
            collective_id=0, has_side_effects=True, vmem_limit_bytes=60000 * 1024
        ),
        name="march",
    )(
        phase_lag.T,
        flow_state,
        face_weights,
        forcing,
        lagged_planes,
        face_map,
        surface_record,
        face_radius,
        face_angle,
        face_axial,
        face_stagger,
        face_area,
        listeners,
        observer_group.reshape(1, observers),
    )
    return deliver(field, acoustic.reshape(per, times), signal)


def solution(mesh):
    return jax.shard_map(
        functools.partial(on_device, mesh.shape["pass"], mesh.shape["cell"]),
        mesh=mesh,
        in_specs=(
            P("pass", "cell"),
            P(None, "pass", "cell"),
            P("pass", "cell"),
            P("pass", None, "cell"),
            P(),
            P("pass", "cell"),
            P("pass", None, "cell"),
            P(None, "cell"),
            P(None, "cell"),
            P(None, "cell"),
            P(None, "cell"),
            P(None, "cell"),
            P(),
            P(),
        ),
        out_specs=(P("pass", "cell"), P("cell", None), P()),
        check_vma=False,
    )
```
